32 devices in a mesh: dp: 8 (over z, x), ctx: 2 (over y), tensor: 2 (over core).
Axes of the slice: x: 2, y: 2, z: 4, core: 2. Of those that a mesh axis runs over, the one named last changes fastest.
Arguments:
- block_input: bfloat16 [8, 256, 2304], P('dp', ('ctx', 'tensor')), may hold values from -6 to 6
- segment_ids: int32 [8, 256], P('dp'), may hold values from 0 to 5, as said below
- positions: int32 [8, 256], P('dp'), may hold values from 0 to 511, as said below
- query_weight: bfloat16 [2304, 2048], P(('dp', 'ctx'), 'tensor'), may hold values from -0.125 to 0.125
- key_weight: bfloat16 [2304, 1024], P(('dp', 'ctx'), 'tensor'), may hold values from -0.125 to 0.125
- value_weight: bfloat16 [2304, 1024], P(('dp', 'ctx'), 'tensor'), may hold values from -0.125 to 0.125
- output_weight: bfloat16 [2304, 2048], P(('dp', 'ctx'), 'tensor'), may hold values from -0.125 to 0.125
- gate_weight: bfloat16 [2304, 9216], P(('dp', 'ctx'), 'tensor'), may hold values from -0.125 to 0.125
- up_weight: bfloat16 [2304, 9216], P(('dp', 'ctx'), 'tensor'), may hold values from -0.125 to 0.125
- down_weight: bfloat16 [2304, 9216], P(('dp', 'ctx'), 'tensor'), may hold values from -0.0625 to 0.0625
- pre_attention_gain: float32 [2304], replicated, may hold values from 0.25 to 1.75
- post_attention_gain: float32 [2304], replicated, may hold values from 0.25 to 1.75
- pre_feedforward_gain: float32 [2304], replicated, may hold values from 0.25 to 1.75
- post_feedforward_gain: float32 [2304], replicated, may hold values from 0.25 to 1.75
- output_cotangent: bfloat16 [8, 256, 2304], P('dp', ('ctx', 'tensor')), may hold values from -6 to 6
Outputs:
- block_output: bfloat16 [8, 256, 2304], P('dp', ('ctx', 'tensor'))
- input_grad: bfloat16 [8, 256, 2304], P('dp', ('ctx', 'tensor'))
- query_grad: float32 [2304, 2048], P(('dp', 'ctx'), 'tensor')
- key_grad: float32 [2304, 1024], P(('dp', 'ctx'), 'tensor')
- value_grad: float32 [2304, 1024], P(('dp', 'ctx'), 'tensor')
- output_grad: float32 [2304, 2048], P(('dp', 'ctx'), 'tensor')
- gate_grad: float32 [2304, 9216], P(('dp', 'ctx'), 'tensor')
- up_grad: float32 [2304, 9216], P(('dp', 'ctx'), 'tensor')
- down_grad: float32 [2304, 9216], P(('dp', 'ctx'), 'tensor')
- pre_attention_grad: float32 [2304], replicated
- post_attention_grad: float32 [2304], replicated
- pre_feedforward_grad: float32 [2304], replicated
- post_feedforward_grad: float32 [2304], replicated
The draws below stay inside these ranges and needn't reach their ends.
Inputs may be any that keep to these rules, and one draw needn't show every extreme that they name: `segment_ids`: in each sequence segment ids start at 0 and never fall; every sequence holds two documents or more. Inside a document positions rise by one from token to token; every document but the first of its sequence starts at position 0.
All inputs are finite; a program needn't handle non-finite values.
Results may differ from the reference program's by a relative error of at most 0.03.
Values may be sent and summed in bfloat16 or wider, within the bound.
A program may use at most 256 MiB of HBM per device.

```python
import math
import jax
import jax.numpy as jnp
from jax import lax

D = 2304
HEADS = 8
KV_HEADS = 4
HEAD_DIM = 256
FF = 9216
LENGTH = 256
SEQS = 8
N_CTX = 2
N_TENSOR = 2


def doc_layout(key):
    base = jax.random.fold_in(key, 11)
    first_key, rest_key, offset_key = jax.random.split(base, 3)
    row_index = jnp.arange(SEQS)[:, None]
    first_len = jax.random.randint(first_key, (SEQS, 1), 1, LENGTH // 2 + 1)
    first_len = jnp.where(row_index == 0, 1, first_len)
    rest_len = jax.random.randint(rest_key, (SEQS, 7), LENGTH // 5 + 1, 2 * LENGTH + 1)
    rest_len = jnp.where(row_index == 0, LENGTH // 5 + 1, rest_len)
    bounds = jnp.concatenate([first_len, first_len + jnp.cumsum(rest_len, axis=1)], axis=1)
    ladder = jnp.arange(LENGTH)
    passed = bounds[:, None, :] <= ladder[None, :, None]
    seg_ids = jnp.sum(passed.astype(jnp.int32), axis=2)
    starts = jnp.max(jnp.where(passed, bounds[:, None, :], 0), axis=2)
    carry_in = jax.random.randint(offset_key, (SEQS, 1), 0, 2 * LENGTH - LENGTH // 2)
    carry_in = jnp.where(row_index == 0, 2 * LENGTH - 1, carry_in)
    token_pos = ladder[None, :] - starts + jnp.where(seg_ids == 0, carry_in, 0)
    return (seg_ids.astype(jnp.int32), token_pos.astype(jnp.int32))


def draw_segment_ids(key, part):
    return doc_layout(key)[0]


def draw_positions(key, part):
    return doc_layout(key)[1]


def with_spikes(array, rng, source, target, shards_of, factor):
    def block_of(dim):
        return (jnp.arange(array.shape[dim]) // (array.shape[dim] // shards_of)).reshape((-1,) + (1,) * (array.ndim - 1 - dim))

    one_side = jax.random.permutation(rng, shards_of)[block_of(target)]
    far = (block_of(target) + shards_of // 2) % shards_of
    return jnp.where((block_of(source) == one_side) | (block_of(source) == far), factor * array, array)


def steps_of(rng, shape, pieces, low, top_value):
    factor_of, own = 1.0, jax.random.fold_in(rng, 6)
    for dim, blocks in pieces:
        steps = jnp.exp(jax.random.uniform(jax.random.fold_in(own, dim), (blocks,), jnp.float32, low / len(pieces), top_value / len(pieces)))
        factor_of = factor_of * jnp.repeat(steps, shape[dim] // blocks).reshape([-1 if axis == dim else 1 for axis in range(len(shape))])
    return factor_of


def bell_draw(rng, shape, scale, bound, cuts=(), kind=jnp.bfloat16):
    level = steps_of(rng, shape, cuts, -0.22, 0.18) if cuts else 1.0
    array = jax.random.normal(rng, shape, jnp.float32) * scale * level
    return jnp.minimum(jnp.maximum(array, -bound), bound).astype(kind)


def bell_draw_with(stream_key, extent, spread, limit, shards, heavy, kind=jnp.bfloat16):
    entries = spread * jax.random.normal(stream_key, extent, jnp.float32)
    if shards:
        entries = entries * steps_of(stream_key, extent, shards, -0.22, 0.18)
    return jnp.clip(with_spikes(entries, jax.random.fold_in(stream_key, 3), *heavy), -limit, limit).astype(kind)


def setup_inputs(seed: int = 0) -> dict:
    arg_keys = jax.random.split(jax.random.key(seed), 16)
    return {
        "block_input": bell_draw(arg_keys[0], (SEQS, LENGTH, D), 1.0, 6.0, ((0, 8), (1, 4))),
        "segment_ids": draw_segment_ids(jax.random.fold_in(arg_keys[15], 71), 0),
        "positions": draw_positions(jax.random.fold_in(arg_keys[15], 71), 0),
        "query_weight": bell_draw(arg_keys[3], (D, HEADS * HEAD_DIM), D ** -0.5, 0.125, ((0, 16), (1, 2))),
        "key_weight": bell_draw(arg_keys[4], (D, KV_HEADS * HEAD_DIM), D ** -0.5, 0.125, ((0, 16), (1, 2))),
        "value_weight": bell_draw(arg_keys[5], (D, KV_HEADS * HEAD_DIM), D ** -0.5, 0.125, ((0, 16), (1, 2))),
        "output_weight": bell_draw(arg_keys[6], (D, HEADS * HEAD_DIM), (HEADS * HEAD_DIM) ** -0.5, 0.125, ((0, 16), (1, 2))),
        "gate_weight": bell_draw(arg_keys[7], (D, FF), D ** -0.5, 0.125, ((0, 16), (1, 2))),
        "up_weight": bell_draw(arg_keys[8], (D, FF), D ** -0.5, 0.125, ((0, 16), (1, 2))),
        "down_weight": bell_draw(arg_keys[9], (D, FF), FF ** -0.5, 0.0625, ((0, 16), (1, 2))),
        "pre_attention_gain": jnp.clip(1.0 + 0.15 * jax.random.normal(arg_keys[10], (D,), jnp.float32), 0.25, 1.75),
        "post_attention_gain": jnp.clip(1.0 + 0.15 * jax.random.normal(arg_keys[11], (D,), jnp.float32), 0.25, 1.75),
        "pre_feedforward_gain": jnp.clip(1.0 + 0.15 * jax.random.normal(arg_keys[12], (D,), jnp.float32), 0.25, 1.75),
        "post_feedforward_gain": jnp.clip(1.0 + 0.15 * jax.random.normal(arg_keys[13], (D,), jnp.float32), 0.25, 1.75),
        "output_cotangent": bell_draw_with(arg_keys[14], (SEQS, LENGTH, D), 1.0, 6.0, ((0, 8), (1, 4)), (0, 2, 8, 2.0)),
    }


EPS = 1e-06
CAP = 50.0
ROPE_BASE = 10000.0
GELU_SCALE = math.sqrt(2.0 / math.pi)
GELU_CUBE = 0.044715

def rms_scale(values):
    return lax.rsqrt(lax.optimization_barrier(jnp.mean(values * values, axis=-1, keepdims=True)) + EPS)

def norm_back(upstream, inputs, scale, gain):
    scaled = gain * upstream
    return scale * scaled - inputs * (scale * scale * scale) * lax.optimization_barrier(jnp.mean(scaled * inputs, axis=-1, keepdims=True))

def rope_tables(token_pos, head_width):
    halfway = head_width // 2
    ladder = jnp.arange(halfway).astype(jnp.float32)
    freqs = jnp.exp(ladder * (-2.0 * math.log(ROPE_BASE) / head_width))
    angles = token_pos.astype(jnp.float32)[:, None] * freqs[None, :]
    return (jnp.cos(angles), jnp.sin(angles))

def rotate(values, cosine, sine):
    halfway = values.shape[-1] // 2
    first_half = values[..., :halfway]
    second_half = values[..., halfway:]
    cos_wide = cosine[:, None, :]
    sin_wide = sine[:, None, :]
    return jnp.concatenate([first_half * cos_wide - second_half * sin_wide, second_half * cos_wide + first_half * sin_wide], axis=-1)

def gelu_parts(gate_vals):
    inner = GELU_SCALE * (gate_vals + GELU_CUBE * gate_vals * gate_vals * gate_vals)
    bend = jnp.tanh(inner)
    value = 0.5 * gate_vals * (1.0 + bend)
    slope = 0.5 * (1.0 + bend) + 0.5 * gate_vals * (1.0 - bend * bend) * GELU_SCALE * (1.0 + 3.0 * GELU_CUBE * gate_vals * gate_vals)
    return (value, slope)

def to_low(values):
    return lax.optimization_barrier(values.astype(jnp.bfloat16))

def low_wide(values):
    return to_low(values).astype(jnp.float32)

def matmul(left, right):
    return jnp.dot(left, right, preferred_element_type=jnp.float32)

def reference(block_input, segment_ids, positions, query_weight, key_weight, value_weight, output_weight, gate_weight, up_weight, down_weight, pre_attention_gain, post_attention_gain, pre_feedforward_gain, post_feedforward_gain, output_cotangent):
    per_group = HEADS // KV_HEADS
    query_scale = HEAD_DIM ** (-0.5)
    q_cols = HEADS * HEAD_DIM // N_TENSOR
    k_cols = KV_HEADS * HEAD_DIM // N_TENSOR
    f_cols = FF // N_TENSOR
    half_len = LENGTH // N_CTX
    weights = (query_weight, key_weight, value_weight, output_weight, gate_weight, up_weight, down_weight)
    gains = (pre_attention_gain, post_attention_gain, pre_feedforward_gain, post_feedforward_gain)

    def one_sequence(totals, slices):
        tokens, seg_row, pos_row, cotan = slices
        resid = tokens.astype(jnp.float32)
        scale_attn = rms_scale(resid)
        attn_input = to_low(resid * scale_attn * pre_attention_gain)
        cosine, sine = rope_tables(pos_row, HEAD_DIM)
        query_lin = matmul(attn_input, query_weight).reshape(LENGTH, HEADS, HEAD_DIM)
        key_lin = matmul(attn_input, key_weight).reshape(LENGTH, KV_HEADS, HEAD_DIM)
        value_lin = matmul(attn_input, value_weight).reshape(LENGTH, KV_HEADS, HEAD_DIM)
        query_rot = to_low(rotate(query_lin, cosine, sine) * query_scale)
        key_rot = to_low(rotate(key_lin, cosine, sine))
        value_low = to_low(value_lin)
        query_grouped = query_rot.reshape(LENGTH, KV_HEADS, per_group, HEAD_DIM).astype(jnp.float32)
        key_wide = key_rot.astype(jnp.float32)
        value_wide = value_low.astype(jnp.float32)
        raw_scores = jnp.einsum('qkgd,skd->kgqs', query_grouped, key_wide)
        bent = jnp.tanh(raw_scores / CAP)
        capped = CAP * bent
        ladder = jnp.arange(LENGTH)
        allowed = (ladder[None, :] <= ladder[:, None]) & (seg_row[None, :] == seg_row[:, None])
        log_total = jnp.log(lax.optimization_barrier(jnp.sum(jnp.where(allowed, jnp.exp(capped), 0.0), axis=-1, keepdims=True)))
        probs = jnp.where(allowed, jnp.exp(capped - log_total), 0.0)
        probs_low = to_low(probs).astype(jnp.float32)
        mixed = jnp.einsum('kgqs,skd->qkgd', probs_low, value_wide)
        mixed_low = to_low(mixed.reshape(LENGTH, HEADS * HEAD_DIM))
        attn_out = jnp.zeros((LENGTH, D), jnp.float32)
        for group in range(N_TENSOR):
            cols = slice(group * q_cols, (group + 1) * q_cols)
            attn_out = attn_out + low_wide(matmul(mixed_low[:, cols], output_weight[:, cols].T))
        scale_post = rms_scale(attn_out)
        hidden = resid + attn_out * scale_post * post_attention_gain
        scale_ffn = rms_scale(hidden)
        ffn_input = to_low(hidden * scale_ffn * pre_feedforward_gain)
        gate_lin = matmul(ffn_input, gate_weight)
        up_lin = matmul(ffn_input, up_weight)
        gelu_value, gelu_slope = gelu_parts(gate_lin)
        product = to_low(gelu_value * up_lin)
        ffn_out = jnp.zeros((LENGTH, D), jnp.float32)
        for group in range(N_TENSOR):
            cols = slice(group * f_cols, (group + 1) * f_cols)
            ffn_out = ffn_out + low_wide(matmul(product[:, cols], down_weight[:, cols].T))
        scale_out = rms_scale(ffn_out)
        block_out = (hidden + ffn_out * scale_out * post_feedforward_gain).astype(jnp.bfloat16)
        upstream = cotan.astype(jnp.float32)
        grad_post_ffn = lax.optimization_barrier(jnp.sum(upstream * ffn_out * scale_out, axis=0))
        d_ffn_out = to_low(norm_back(upstream, ffn_out, scale_out, post_feedforward_gain))
        d_product = matmul(d_ffn_out, down_weight)
        down_grad = matmul(d_ffn_out.T, product)
        d_gate = to_low(d_product * up_lin * gelu_slope)
        d_up = to_low(d_product * gelu_value)
        gate_grad = matmul(ffn_input.T, d_gate)
        up_grad = matmul(ffn_input.T, d_up)
        d_ffn_input = jnp.zeros((LENGTH, D), jnp.float32)
        for group in range(N_TENSOR):
            cols = slice(group * f_cols, (group + 1) * f_cols)
            term = matmul(d_gate[:, cols], gate_weight[:, cols].T) + matmul(d_up[:, cols], up_weight[:, cols].T)
            d_ffn_input = d_ffn_input + low_wide(term)
        grad_pre_ffn = lax.optimization_barrier(jnp.sum(d_ffn_input * hidden * scale_ffn, axis=0))
        d_hidden = upstream + norm_back(d_ffn_input, hidden, scale_ffn, pre_feedforward_gain)
        grad_post_attn = lax.optimization_barrier(jnp.sum(d_hidden * attn_out * scale_post, axis=0))
        d_attn_out = to_low(norm_back(d_hidden, attn_out, scale_post, post_attention_gain))
        output_grad = matmul(d_attn_out.T, mixed_low)
        d_mixed = matmul(d_attn_out, output_weight).reshape(LENGTH, KV_HEADS, per_group, HEAD_DIM)
        d_mixed_low = to_low(d_mixed).astype(jnp.float32)
        delta = jnp.einsum('qkgd,qkgd->kgq', d_mixed, mixed)[..., None]
        d_probs = jnp.einsum('qkgd,skd->kgqs', d_mixed_low, value_wide)
        d_scores = to_low(probs * (d_probs - delta) * (1.0 - bent * bent)).astype(jnp.float32)
        d_query = jnp.einsum('kgqs,skd->qkgd', d_scores, key_wide).reshape(LENGTH, HEADS, HEAD_DIM)
        d_query_low = to_low(rotate(d_query, cosine, -sine) * query_scale).reshape(LENGTH, HEADS * HEAD_DIM)
        d_key = jnp.zeros((LENGTH, KV_HEADS, HEAD_DIM), jnp.float32)
        d_value = jnp.zeros((LENGTH, KV_HEADS, HEAD_DIM), jnp.float32)
        for half in range(N_CTX):
            rows = slice(half * half_len, (half + 1) * half_len)
            d_key = d_key + low_wide(jnp.einsum('kgqs,qkgd->skd', d_scores[:, :, rows, :], query_grouped[rows]))
            d_value = d_value + low_wide(jnp.einsum('kgqs,qkgd->skd', probs_low[:, :, rows, :], d_mixed_low[rows]))
        d_key_low = to_low(rotate(d_key, cosine, -sine)).reshape(LENGTH, KV_HEADS * HEAD_DIM)
        d_value_low = to_low(d_value).reshape(LENGTH, KV_HEADS * HEAD_DIM)
        query_grad = matmul(attn_input.T, d_query_low)
        key_grad = matmul(attn_input.T, d_key_low)
        value_grad = matmul(attn_input.T, d_value_low)
        d_attn_input = jnp.zeros((LENGTH, D), jnp.float32)
        for group in range(N_TENSOR):
            qc = slice(group * q_cols, (group + 1) * q_cols)
            kc = slice(group * k_cols, (group + 1) * k_cols)
            term = matmul(d_query_low[:, qc], query_weight[:, qc].T)
            term = term + matmul(d_key_low[:, kc], key_weight[:, kc].T)
            term = term + matmul(d_value_low[:, kc], value_weight[:, kc].T)
            d_attn_input = d_attn_input + low_wide(term)
        grad_pre_attn = lax.optimization_barrier(jnp.sum(d_attn_input * resid * scale_attn, axis=0))
        input_grad = (d_hidden + norm_back(d_attn_input, resid, scale_attn, pre_attention_gain)).astype(jnp.bfloat16)
        terms = (query_grad, key_grad, value_grad, output_grad, gate_grad, up_grad, down_grad, grad_pre_attn, grad_post_attn, grad_pre_ffn, grad_post_ffn)
        new_totals = tuple((total + term for total, term in zip(totals, terms)))
        return (new_totals, (block_out, input_grad))
    start = tuple((jnp.zeros(item.shape, jnp.float32) for item in weights + gains))
    totals, stacked = lax.scan(one_sequence, start, (block_input, segment_ids, positions, output_cotangent))
    return (stacked[0], stacked[1], totals[0], totals[1], totals[2], totals[3], totals[4], totals[5], totals[6], totals[7], totals[8], totals[9], totals[10])
```

```python
import math

import jax
import jax.numpy as jnp
from jax import lax
from jax.sharding import Mesh, PartitionSpec as P

HEAD_DIM = 256
LINE = 4
PAIR = 2

EPS = 1e-06
CAP = 50.0
ROPE_BASE = 10000.0
GELU_SCALE = math.sqrt(2.0 / math.pi)
GELU_CUBE = 0.044715


def low(values):
    return values.astype(jnp.bfloat16)


def wide(values):
    return values.astype(jnp.float32)


def rms_scale(values):
    return lax.rsqrt(jnp.mean(values * values, axis=-1, keepdims=True) + EPS)


def norm_back(upstream, inputs, scale, gain):
    scaled = gain * upstream
    return scale * scaled - inputs * (scale * scale * scale) * jnp.mean(
        scaled * inputs, axis=-1, keepdims=True
    )


def rope_tables(token_pos, head_width):
    halfway = head_width // 2
    ladder = jnp.arange(halfway).astype(jnp.float32)
    freqs = jnp.exp(ladder * (-2.0 * math.log(ROPE_BASE) / head_width))
    angles = token_pos.astype(jnp.float32)[:, None] * freqs[None, :]
    return (jnp.cos(angles), jnp.sin(angles))


def rotate(values, cosine, sine):
    halfway = values.shape[-1] // 2
    first_half = values[..., :halfway]
    second_half = values[..., halfway:]
    return jnp.concatenate(
        [
            first_half * cosine - second_half * sine,
            second_half * cosine + first_half * sine,
        ],
        axis=-1,
    )


def gelu_parts(gate_vals):
    inner = GELU_SCALE * (gate_vals + GELU_CUBE * gate_vals * gate_vals * gate_vals)
    bend = jnp.tanh(inner)
    value = 0.5 * gate_vals * (1.0 + bend)
    slope = 0.5 * (1.0 + bend) + 0.5 * gate_vals * (1.0 - bend * bend) * GELU_SCALE * (
        1.0 + 3.0 * GELU_CUBE * gate_vals * gate_vals
    )
    return (value, slope)


def matmul(left, right):
    return jnp.dot(left, right, preferred_element_type=jnp.float32)


def matmul_nt(left, right):
    return lax.dot_general(
        left, right, (((1,), (1,)), ((), ())), preferred_element_type=jnp.float32
    )


def matmul_tn(left, right):
    return lax.dot_general(
        left, right, (((0,), (0,)), ((), ())), preferred_element_type=jnp.float32
    )


def swap(values, axis):
    return lax.ppermute(values, axis, [(0, 1), (1, 0)])


def shift(values, hops):
    return lax.ppermute(values, "z", [(i, (i + hops) % LINE) for i in range(LINE)])


def flip(values, code):
    return lax.ppermute(values, ("x", "y"), [(i, i ^ code) for i in range(4)])


def over_m(values):
    if lax.axis_size("m") == 1:
        return values[None]
    return lax.all_gather(values, "m", axis=0)


def reduce_m(values):
    if lax.axis_size("m") == 1:
        return values[0]
    return low(lax.psum_scatter(values, "m", scatter_dimension=0, tiled=False))


def in_order(own, other, index, axis):
    pair = jnp.stack([own, other], axis)
    turned = jnp.stack([other, own], axis)
    return jnp.where(index == 0, pair, turned)


def put(buffer, block, **where):
    names = "zmxyrc"
    start = [where.get(name, 0) for name in names[: buffer.ndim]]
    return lax.dynamic_update_slice(buffer, block, start)


def fetch_ffn(weight, place, turn):
    z, x, y = place
    rows, cols = weight.shape
    quarter = cols // LINE
    pieces = []
    for hops in range(LINE):
        target = (z + hops) % LINE
        part = lax.dynamic_slice_in_dim(weight, target * quarter, quarter, 1)
        pieces.append(part if hops == 0 else shift(part, hops))
    count = lax.axis_size("m")
    buffer = jnp.zeros((LINE, count, PAIR, PAIR, rows, quarter), weight.dtype)
    for hops, piece in enumerate(pieces):
        source = (z - hops) % LINE
        piece = over_m(piece)
        if (hops + turn) % 2 == 0:
            pair = in_order(piece, swap(piece, "x"), x, 1)
            far = swap(pair, "y")
            buffer = put(buffer, pair[None, :, :, None], z=source, y=y)
            buffer = put(buffer, far[None, :, :, None], z=source, y=1 - y)
        else:
            pair = in_order(piece, swap(piece, "y"), y, 1)
            far = swap(pair, "x")
            buffer = put(buffer, pair[None, :, None], z=source, x=x)
            buffer = put(buffer, far[None, :, None], z=source, x=1 - x)
    return buffer.reshape(-1, quarter)


def fetch_attn(cut, place):
    z, x, y = place
    own = cut(x, y)
    rows, cols = own.shape
    block = jnp.zeros((PAIR, PAIR, rows, cols), own.dtype)
    block = lax.dynamic_update_slice(block, own[None, None], (x, y, 0, 0))
    for code in range(1, 4):
        dx, dy = code // 2, code % 2
        got = flip(cut(x ^ dx, y ^ dy), code)
        block = lax.dynamic_update_slice(block, got[None, None], (x ^ dx, y ^ dy, 0, 0))
    block = over_m(block)
    buffer = jnp.zeros((LINE,) + block.shape, own.dtype)
    buffer = put(buffer, block[None], z=z)
    for hops in range(1, LINE):
        buffer = put(buffer, shift(block, hops)[None], z=(z - hops) % LINE)
    return buffer.reshape(-1, cols)


def return_ffn(partial, place):
    z, x, y = place
    quarter = partial.shape[-1]
    count = lax.axis_size("m")
    blocks = partial.reshape(LINE, count, PAIR, PAIR, -1, quarter)
    half = LINE // 2

    def pick(values, index, axis):
        return lax.dynamic_index_in_dim(values, index, axis, keepdims=False)

    first, second = blocks[:half], blocks[half:]
    first = low(wide(pick(first, x, 2)) + wide(swap(pick(first, 1 - x, 2), "x")))
    second = low(wide(pick(second, y, 3)) + wide(swap(pick(second, 1 - y, 3), "y")))
    first = wide(pick(first, y, 2)) + wide(swap(pick(first, 1 - y, 2), "y"))
    second = wide(pick(second, x, 2)) + wide(swap(pick(second, 1 - x, 2), "x"))
    total = low(jnp.concatenate([first, second], 0))
    total = reduce_m(jnp.swapaxes(total, 0, 1))
    rows = total.shape[1]
    out = jnp.zeros((rows, LINE * quarter), jnp.float32)
    for hops in range(LINE):
        part = pick(total, (z + hops) % LINE, 0)
        part = part if hops == 0 else shift(part, hops)
        out = lax.dynamic_update_slice(out, wide(part), (0, ((z - hops) % LINE) * quarter))
    return out


def return_attn(partial, place):
    z, x, y = place
    cols = partial.shape[-1]
    count = lax.axis_size("m")
    blocks = partial.reshape(LINE, count, PAIR, PAIR, -1, cols)

    def pick(values, index):
        return lax.dynamic_index_in_dim(values, index, 0, keepdims=False)

    total = wide(pick(blocks, z))
    for hops in range(1, LINE):
        total = total + wide(shift(pick(blocks, (z + hops) % LINE), hops))
    total = reduce_m(low(total))
    total = total.reshape(4, -1, cols)
    me = x * 2 + y
    return [wide(pick(total, me))] + [
        wide(flip(pick(total, me ^ code), code)) for code in range(1, 4)
    ]


def spread_line(rows):
    near = jnp.concatenate([rows] + [shift(rows, hops) for hops in range(1, LINE)], 0)
    return jnp.concatenate([near, swap(near, "c")], 0)


def gather_line(partial):
    half = partial.shape[0] // 2
    near = wide(partial[:half]) + wide(swap(low(partial[half:]), "c"))
    pieces = near.reshape(LINE, half // LINE, -1)
    total = pieces[0]
    for hops in range(1, LINE):
        total = total + wide(shift(low(pieces[hops]), -hops))
    return total


def spread_plane(rows):
    mine = [rows] + [flip(rows, code) for code in range(1, 4)]
    out = []
    for dx in range(2):
        near = jnp.concatenate(mine[2 * dx : 2 * dx + 2], 0)
        out += [near, swap(near, "c")]
    return jnp.concatenate(out, 0)


def gather_plane(partial):
    count = partial.shape[0] // 8
    blocks = partial.reshape(2, 2, 2, count, -1)
    near = wide(blocks[:, 0]) + wide(swap(low(blocks[:, 1]), "c"))
    total = near[0, 0]
    for code in range(1, 4):
        total = total + wide(flip(low(near[code // 2, code % 2]), code))
    return total


def sum_everywhere(values):
    values = values + swap(values, "c")
    values = values + swap(values, "x")
    values = values + swap(values, "y")
    for code in (1, 2):
        values = values + lax.ppermute(values, "z", [(i, i ^ code) for i in range(LINE)])
    if lax.axis_size("m") > 1:
        values = lax.psum(values, "m")
    return values


def body(
    block_input,
    segment_ids,
    positions,
    query_weight,
    key_weight,
    value_weight,
    output_weight,
    gate_weight,
    up_weight,
    down_weight,
    pre_attention_gain,
    post_attention_gain,
    pre_feedforward_gain,
    post_feedforward_gain,
    output_cotangent,
):
    z, x, y, c = (lax.axis_index(name) for name in "zxyc")
    place = (z, x, y)
    query_scale = HEAD_DIM ** (-0.5)
    count = block_input.shape[1]
    seq_len = segment_ids.shape[1]

    def head(weight, index):
        return lax.dynamic_slice_in_dim(weight, index * HEAD_DIM, HEAD_DIM, 1)

    def cut_qkv(to_x, to_y):
        mixed_in = jnp.where(to_x == 0, head(key_weight, to_y), head(value_weight, to_y))
        return jnp.concatenate([head(query_weight, to_y * 2 + to_x), mixed_in], 1)

    def cut_out(to_x, to_y):
        return head(output_weight, to_y * 2 + to_x)

    resid = wide(block_input[0])
    scale_attn = rms_scale(resid)
    attn_rows = low(resid * scale_attn * pre_attention_gain)
    attn_input = spread_plane(attn_rows)
    qkv_full = fetch_attn(cut_qkv, place)
    out_full = fetch_attn(cut_out, place)
    gate_full = fetch_ffn(gate_weight, place, 0)
    up_full = fetch_ffn(up_weight, place, 1)
    down_full = fetch_ffn(down_weight, place, 0)

    tags = jnp.stack([segment_ids[0], positions[0]])
    tags = jnp.stack([tags, swap(tags, "x")])
    starts = [((y ^ dy) * 2 + (c ^ dc)) * count for dc in range(2) for dy in range(2)]
    tags = jnp.concatenate(
        [lax.dynamic_slice_in_dim(tags, start, count, 2) for start in starts], 2
    )
    order = jnp.concatenate([start + jnp.arange(count) for start in starts])
    seg, pos = tags[:, 0], tags[:, 1]
    allowed = (order[None, :] <= order[:, None])[None] & (seg[:, None, :] == seg[:, :, None])
    cosine, sine = rope_tables(pos.reshape(-1), HEAD_DIM)

    def per_seq(values):
        return values.reshape(2, seq_len, HEAD_DIM)

    def turned(values):
        return values.reshape(2, seq_len, HEAD_DIM)[::-1].reshape(values.shape)

    lin = matmul(attn_input, qkv_full)
    query_lin, other_lin = lin[:, :HEAD_DIM], lin[:, HEAD_DIM:]
    query = per_seq(low(rotate(query_lin, cosine, sine) * query_scale))
    own_kv = low(jnp.where(x == 0, rotate(other_lin, cosine, sine), other_lin))
    far_kv = turned(swap(own_kv, "x"))
    key = per_seq(jnp.where(x == 0, own_kv, far_kv))
    value = per_seq(jnp.where(x == 0, far_kv, own_kv))

    raw = jnp.einsum("bqd,bkd->bqk", query, key, preferred_element_type=jnp.float32)
    bent = jnp.tanh(raw / CAP)
    capped = CAP * bent
    log_total = jnp.log(jnp.sum(jnp.where(allowed, jnp.exp(capped), 0.0), axis=-1, keepdims=True))
    probs = jnp.where(allowed, jnp.exp(capped - log_total), 0.0)
    probs_low = low(probs)
    mixed = jnp.einsum("bqk,bkd->bqd", probs_low, value, preferred_element_type=jnp.float32)
    mixed_low = low(mixed).reshape(-1, HEAD_DIM)
    attn_out = gather_plane(matmul_nt(mixed_low, out_full))
    scale_post = rms_scale(attn_out)
    hidden = resid + attn_out * scale_post * post_attention_gain
    scale_ffn = rms_scale(hidden)
    ffn_rows = low(hidden * scale_ffn * pre_feedforward_gain)

    ffn_input = spread_line(ffn_rows)
    gate_lin = matmul(ffn_input, gate_full)
    up_lin = matmul(ffn_input, up_full)
    gelu_value, gelu_slope = gelu_parts(gate_lin)
    product = low(gelu_value * up_lin)
    ffn_out = gather_line(matmul_nt(product, down_full))
    scale_out = rms_scale(ffn_out)
    block_out = low(hidden + ffn_out * scale_out * post_feedforward_gain)

    upstream = wide(output_cotangent[0])
    grad_post_ffn = jnp.sum(upstream * ffn_out * scale_out, axis=0)
    d_ffn_rows = low(norm_back(upstream, ffn_out, scale_out, post_feedforward_gain))
    d_ffn_out = spread_line(d_ffn_rows)
    d_product = matmul(d_ffn_out, down_full)
    d_gate = low(d_product * up_lin * gelu_slope)
    d_up = low(d_product * gelu_value)
    d_ffn_input = gather_line(matmul_nt(d_gate, gate_full) + matmul_nt(d_up, up_full))
    down_grad = return_ffn(low(matmul_tn(d_ffn_out, product)), place)
    gate_grad = return_ffn(low(matmul_tn(ffn_input, d_gate)), place)
    up_grad = return_ffn(low(matmul_tn(ffn_input, d_up)), place)

    grad_pre_ffn = jnp.sum(d_ffn_input * hidden * scale_ffn, axis=0)
    d_hidden = upstream + norm_back(d_ffn_input, hidden, scale_ffn, pre_feedforward_gain)
    grad_post_attn = jnp.sum(d_hidden * attn_out * scale_post, axis=0)
    d_attn_rows = low(norm_back(d_hidden, attn_out, scale_post, post_attention_gain))
    d_attn_out = spread_plane(d_attn_rows)
    d_mixed = per_seq(matmul(d_attn_out, out_full))
    d_mixed_low = low(d_mixed)
    delta = jnp.sum(d_mixed * mixed, axis=-1, keepdims=True)
    d_probs = jnp.einsum("bqd,bkd->bqk", d_mixed_low, value, preferred_element_type=jnp.float32)
    d_scores = low(probs * (d_probs - delta) * (1.0 - bent * bent))
    d_query = jnp.einsum("bqk,bkd->bqd", d_scores, key, preferred_element_type=jnp.float32)
    d_key = jnp.einsum("bqk,bqd->bkd", d_scores, query, preferred_element_type=jnp.float32)
    d_value = jnp.einsum("bqk,bqd->bkd", probs_low, d_mixed_low, preferred_element_type=jnp.float32)
    d_query_low = low(rotate(d_query.reshape(-1, HEAD_DIM), cosine, -sine) * query_scale)
    keep = jnp.where(x == 0, d_key, d_value).reshape(-1, HEAD_DIM)
    give = low(jnp.where(x == 0, d_value, d_key)).reshape(-1, HEAD_DIM)
    d_kv = keep + wide(turned(swap(give, "x")))
    d_kv_low = low(jnp.where(x == 0, rotate(d_kv, cosine, -sine), d_kv))
    d_qkv = jnp.concatenate([d_query_low, d_kv_low], 1)
    d_attn_input = gather_plane(matmul_nt(d_qkv, qkv_full))
    grad_pre_attn = jnp.sum(d_attn_input * resid * scale_attn, axis=0)
    input_grad = low(d_hidden + norm_back(d_attn_input, resid, scale_attn, pre_attention_gain))

    out_parts = return_attn(low(matmul_tn(d_attn_out, mixed_low)), place)
    qkv_parts = return_attn(low(matmul_tn(attn_input, d_qkv)), place)

    def ordered(parts):
        grid = jnp.stack(parts).reshape((2, 2) + parts[0].shape)
        grid = jnp.where(x == 0, grid, grid[::-1])
        return jnp.where(y == 0, grid, grid[:, ::-1])

    def heads(grid):
        return jnp.concatenate([grid[0, 0], grid[1, 0], grid[0, 1], grid[1, 1]], 1)

    output_grad = heads(ordered(out_parts))
    qkv_grid = ordered(qkv_parts)
    query_grad = heads(qkv_grid[..., :HEAD_DIM])
    key_grad = jnp.concatenate([qkv_grid[0, 0], qkv_grid[0, 1]], 1)
    rest = qkv_grid[..., HEAD_DIM:]
    key_grad = jnp.concatenate([rest[0, 0], rest[0, 1]], 1)
    value_grad = jnp.concatenate([rest[1, 0], rest[1, 1]], 1)

    gain_sums = sum_everywhere(
        jnp.stack([grad_pre_attn, grad_post_attn, grad_pre_ffn, grad_post_ffn])
    )
    return (
        block_out[None],
        input_grad[None],
        query_grad,
        key_grad,
        value_grad,
        output_grad,
        gate_grad,
        up_grad,
        down_grad,
        gain_sums[0],
        gain_sums[1],
        gain_sums[2],
        gain_sums[3],
    )


def solution(mesh):
    dp, ctx, tensor = (mesh.shape[name] for name in ("dp", "ctx", "tensor"))
    shape = (LINE, dp // (LINE * PAIR), PAIR, ctx, tensor)
    fine = Mesh(mesh.devices.reshape(shape), ("z", "m", "x", "y", "c"))
    seqs = ("z", "m", "x")
    tokens = P(seqs, ("y", "c"), None)
    weight = P(seqs + ("y",), "c")
    in_specs = (tokens, P(seqs, None), P(seqs, None)) + (weight,) * 7 + (P(),) * 4 + (tokens,)
    out_specs = (tokens, tokens) + (weight,) * 7 + (P(),) * 4
    return jax.shard_map(body, mesh=fine, in_specs=in_specs, out_specs=out_specs, check_vma=False)
```

```python
import math

import jax
import jax.numpy as jnp
from jax import lax
from jax.sharding import Mesh, PartitionSpec as P

HEAD_DIM = 256
LINE = 4
PAIR = 2

EPS = 1e-06
CAP = 50.0
ROPE_BASE = 10000.0
GELU_SCALE = math.sqrt(2.0 / math.pi)
GELU_CUBE = 0.044715


def low(values):
    return values.astype(jnp.bfloat16)


def wide(values):
    return values.astype(jnp.float32)


def rms_scale(values):
    return lax.rsqrt(jnp.mean(values * values, axis=-1, keepdims=True) + EPS)


def norm_back(upstream, inputs, scale, gain):
    scaled = gain * upstream
    return scale * scaled - inputs * (scale * scale * scale) * jnp.mean(
        scaled * inputs, axis=-1, keepdims=True
    )


def rope_tables(token_pos, head_width):
    halfway = head_width // 2
    ladder = jnp.arange(halfway).astype(jnp.float32)
    freqs = jnp.exp(ladder * (-2.0 * math.log(ROPE_BASE) / head_width))
    angles = token_pos.astype(jnp.float32)[:, None] * freqs[None, :]
    return (jnp.cos(angles), jnp.sin(angles))


def rotate(values, cosine, sine):
    halfway = values.shape[-1] // 2
    first_half = values[..., :halfway]
    second_half = values[..., halfway:]
    return jnp.concatenate(
        [
            first_half * cosine - second_half * sine,
            second_half * cosine + first_half * sine,
        ],
        axis=-1,
    )


def gelu_parts(gate_vals):
    inner = GELU_SCALE * (gate_vals + GELU_CUBE * gate_vals * gate_vals * gate_vals)
    bend = jnp.tanh(inner)
    value = 0.5 * gate_vals * (1.0 + bend)
    slope = 0.5 * (1.0 + bend) + 0.5 * gate_vals * (1.0 - bend * bend) * GELU_SCALE * (
        1.0 + 3.0 * GELU_CUBE * gate_vals * gate_vals
    )
    return (value, slope)


def matmul(left, right):
    return jnp.dot(left, right, preferred_element_type=jnp.float32)


def matmul_nt(left, right):
    return lax.dot_general(
        left, right, (((1,), (1,)), ((), ())), preferred_element_type=jnp.float32
    )


def matmul_tn(left, right):
    return lax.dot_general(
        left, right, (((0,), (0,)), ((), ())), preferred_element_type=jnp.float32
    )


def swap(values, axis):
    with jax.named_scope("swap_" + axis):
        return lax.ppermute(values, axis, [(0, 1), (1, 0)])


def shift(values, hops):
    with jax.named_scope("shift"):
        return lax.ppermute(values, "z", [(i, (i + hops) % LINE) for i in range(LINE)])


def flip(values, code):
    with jax.named_scope("flip"):
        return lax.ppermute(values, ("x", "y"), [(i, i ^ code) for i in range(4)])


def label(name):
    return jax.named_scope(name)


def over_m(values):
    if lax.axis_size("m") == 1:
        return values[None]
    return lax.all_gather(values, "m", axis=0)


def reduce_m(values):
    if lax.axis_size("m") == 1:
        return values[0]
    return low(lax.psum_scatter(values, "m", scatter_dimension=0, tiled=False))


def after(values, *earlier):
    return lax.optimization_barrier((values,) + earlier)[0]


def place_at(buffer, block, start):
    return lax.dynamic_update_slice(buffer, block, start + (0,) * (buffer.ndim - len(start)))


def line_ffn(weight, place):
    z, x, y = place
    rows, cols = weight.shape
    quarter = cols // LINE
    line = jnp.zeros((LINE, rows, quarter), weight.dtype)
    for hops in range(LINE):
        part = lax.dynamic_slice_in_dim(weight, ((z + hops) % LINE) * quarter, quarter, 1)
        part = part if hops == 0 else shift(part, hops)
        line = place_at(line, part[None], ((z - hops) % LINE,))
    return line


def plane_ffn_near(line):
    half = LINE // 2
    line = jnp.swapaxes(over_m(line), 0, 1)
    first, second = line[:half], line[half:]
    return (
        line,
        swap(first, "x"),
        swap(first, "y"),
        swap(second, "y"),
        swap(second, "x"),
    )


def plane_ffn_far(near):
    return near + (swap(near[1], "y"), swap(near[3], "x"))


def plane_ffn_join(parts, place):
    z, x, y = place
    line, first_x, first_y, second_y, second_x, first_xy, second_xy = parts
    half = LINE // 2
    count, rows, quarter = line.shape[1:]
    full = jnp.zeros((LINE, count, PAIR, PAIR, rows, quarter), line.dtype)
    full = place_at(full, line[:, :, None, None], (0, 0, x, y))
    full = place_at(full, first_x[:, :, None, None], (0, 0, 1 - x, y))
    full = place_at(full, first_y[:, :, None, None], (0, 0, x, 1 - y))
    full = place_at(full, first_xy[:, :, None, None], (0, 0, 1 - x, 1 - y))
    full = place_at(full, second_x[:, :, None, None], (half, 0, 1 - x, y))
    full = place_at(full, second_y[:, :, None, None], (half, 0, x, 1 - y))
    full = place_at(full, second_xy[:, :, None, None], (half, 0, 1 - x, 1 - y))
    return full.reshape(-1, quarter)


def plane_attn(cut, place):
    z, x, y = place
    own = cut(x, y)
    rows, cols = own.shape
    block = jnp.zeros((PAIR, PAIR, rows, cols), own.dtype)
    block = place_at(block, own[None, None], (x, y))
    for code in range(1, 4):
        dx, dy = code // 2, code % 2
        got = flip(cut(x ^ dx, y ^ dy), code)
        block = place_at(block, got[None, None], (x ^ dx, y ^ dy))
    return block


def line_attn(block, place):
    z, x, y = place
    block = over_m(block)
    buffer = jnp.zeros((LINE,) + block.shape, block.dtype)
    buffer = place_at(buffer, block[None], (z,))
    for hops in range(1, LINE):
        buffer = place_at(buffer, shift(block, hops)[None], ((z - hops) % LINE,))
    return buffer.reshape(-1, block.shape[-1])


def pick(values, index, axis=0):
    return lax.dynamic_index_in_dim(values, index, axis, keepdims=False)


def back_near(partial, place):
    z, x, y = place
    quarter = partial.shape[-1]
    blocks = partial.reshape(LINE, lax.axis_size("m"), PAIR, PAIR, -1, quarter)
    half = LINE // 2
    first, second = blocks[:half], blocks[half:]
    got_first = swap(pick(first, 1 - x, 2), "x")
    got_second = swap(pick(second, 1 - y, 3), "y")
    return pick(first, x, 2), got_first, pick(second, y, 3), got_second


def back_far(near, place):
    z, x, y = place
    own_first, got_first, own_second, got_second = near
    first = low(wide(own_first) + wide(got_first))
    second = low(wide(own_second) + wide(got_second))
    got_first = swap(pick(first, 1 - y, 2), "y")
    got_second = swap(pick(second, 1 - x, 2), "x")
    return pick(first, y, 2), got_first, pick(second, x, 2), got_second


def back_sum(far):
    own_first, got_first, own_second, got_second = far
    first = wide(own_first) + wide(got_first)
    second = wide(own_second) + wide(got_second)
    total = low(jnp.concatenate([first, second], 0))
    return reduce_m(jnp.swapaxes(total, 0, 1))


def back_line(total, place):
    z, x, y = place
    rows, quarter = total.shape[1:]
    out = jnp.zeros((rows, LINE * quarter), jnp.float32)
    for hops in range(LINE):
        part = pick(total, (z + hops) % LINE)
        part = part if hops == 0 else shift(part, hops)
        out = lax.dynamic_update_slice(out, wide(part), (0, ((z - hops) % LINE) * quarter))
    return out


def back_attn_line(partial, place):
    z, x, y = place
    cols = partial.shape[-1]
    blocks = partial.reshape(LINE, lax.axis_size("m"), PAIR, PAIR, -1, cols)
    total = wide(pick(blocks, z))
    for hops in range(1, LINE):
        total = total + wide(shift(pick(blocks, (z + hops) % LINE), hops))
    return reduce_m(low(total)).reshape(4, -1, cols)


def back_attn_plane(total, place):
    z, x, y = place
    me = x * 2 + y
    return [wide(pick(total, me))] + [
        wide(flip(pick(total, me ^ code), code)) for code in range(1, 4)
    ]


def line_near(rows):
    return jnp.concatenate([rows] + [shift(rows, hops) for hops in range(1, LINE)], 0)


def line_far(near):
    return jnp.concatenate([near, swap(near, "c")], 0)


def core_sum(partial):
    half = partial.shape[0] // 2
    return wide(partial[:half]) + wide(swap(low(partial[half:]), "c"))


def line_sum(near):
    pieces = near.reshape(LINE, near.shape[0] // LINE, -1)
    total = pieces[0]
    for hops in range(1, LINE):
        total = total + wide(shift(low(pieces[hops]), -hops))
    return total


def plane_near(rows):
    return tuple([rows] + [flip(rows, code) for code in range(1, 4)])


def plane_far(mine):
    out = []
    for dx in range(2):
        near = jnp.concatenate(mine[2 * dx : 2 * dx + 2], 0)
        out += [near, swap(near, "c")]
    return jnp.concatenate(out, 0)


def plane_core_sum(partial):
    count = partial.shape[0] // 8
    blocks = partial.reshape(2, 2, 2, count, -1)
    return wide(blocks[:, 0]) + wide(swap(low(blocks[:, 1]), "c"))


def plane_sum(near):
    total = near[0, 0]
    for code in range(1, 4):
        total = total + wide(flip(low(near[code // 2, code % 2]), code))
    return total


def sum_everywhere(values):
    values = values + swap(values, "c")
    values = values + swap(values, "x")
    values = values + swap(values, "y")
    for code in (1, 2):
        values = values + lax.ppermute(values, "z", [(i, i ^ code) for i in range(LINE)])
    if lax.axis_size("m") > 1:
        values = lax.psum(values, "m")
    return values


def body(
    block_input,
    segment_ids,
    positions,
    query_weight,
    key_weight,
    value_weight,
    output_weight,
    gate_weight,
    up_weight,
    down_weight,
    pre_attention_gain,
    post_attention_gain,
    pre_feedforward_gain,
    post_feedforward_gain,
    output_cotangent,
):
    z, x, y, c = (lax.axis_index(name) for name in "zxyc")
    place = (z, x, y)
    query_scale = HEAD_DIM ** (-0.5)
    count = block_input.shape[1]
    seq_len = segment_ids.shape[1]

    def head(weight, index):
        return lax.dynamic_slice_in_dim(weight, index * HEAD_DIM, HEAD_DIM, 1)

    def cut_qkv(to_x, to_y):
        mixed_in = jnp.where(to_x == 0, head(key_weight, to_y), head(value_weight, to_y))
        return jnp.concatenate([head(query_weight, to_y * 2 + to_x), mixed_in], 1)

    def cut_out(to_x, to_y):
        return head(output_weight, to_y * 2 + to_x)

    resid = wide(block_input[0])
    scale_attn = rms_scale(resid)
    attn_rows = low(resid * scale_attn * pre_attention_gain)
    with label("gate_z"):
        gate_line = line_ffn(gate_weight, place)
    with label("attn_spread"):
        attn_near = plane_near(attn_rows)
    with label("qkv_plane"):
        qkv_block = plane_attn(cut_qkv, place)
    with label("out_plane"):
        out_block = plane_attn(cut_out, place)
    with label("qkv_z"):
        qkv_full = line_attn(qkv_block, place)
    with label("gate_near"):
        gate_near = plane_ffn_near(gate_line)
    with label("attn_spread"):
        attn_input = plane_far(after(attn_near, gate_line))
    with label("up_z"):
        up_line = line_ffn(after(up_weight, qkv_full), place)

    tags = jnp.stack([segment_ids[0], positions[0]])
    tags = jnp.stack([tags, swap(tags, "x")])
    starts = [((y ^ dy) * 2 + (c ^ dc)) * count for dc in range(2) for dy in range(2)]
    tags = jnp.concatenate(
        [lax.dynamic_slice_in_dim(tags, start, count, 2) for start in starts], 2
    )
    order = jnp.concatenate([start + jnp.arange(count) for start in starts])
    seg, pos = tags[:, 0], tags[:, 1]
    allowed = (order[None, :] <= order[:, None])[None] & (seg[:, None, :] == seg[:, :, None])
    cosine, sine = rope_tables(pos.reshape(-1), HEAD_DIM)

    def per_seq(values):
        return values.reshape(2, seq_len, HEAD_DIM)

    def turned(values):
        return values.reshape(2, seq_len, HEAD_DIM)[::-1].reshape(values.shape)

    lin = matmul(attn_input, qkv_full)
    query_lin, other_lin = lin[:, :HEAD_DIM], lin[:, HEAD_DIM:]
    query = per_seq(low(rotate(query_lin, cosine, sine) * query_scale))
    own_kv = low(jnp.where(x == 0, rotate(other_lin, cosine, sine), other_lin))
    with label("kv"):
        far_kv = swap(own_kv, "x")
    with label("gate_far"):
        gate_far = plane_ffn_far(after(gate_near, own_kv))
    with label("up_near"):
        up_near = plane_ffn_near(after(up_line, gate_near))
    with label("out_z"):
        out_full = line_attn(after(out_block, up_line), place)
    with label("down_z"):
        down_line = line_ffn(after(down_weight, up_line), place)
    far_kv = turned(after(far_kv, up_line, gate_near))
    key = per_seq(jnp.where(x == 0, own_kv, far_kv))
    value = per_seq(jnp.where(x == 0, far_kv, own_kv))

    raw = jnp.einsum("bqd,bkd->bqk", query, key, preferred_element_type=jnp.float32)
    bent = jnp.tanh(raw / CAP)
    capped = CAP * bent
    log_total = jnp.log(jnp.sum(jnp.where(allowed, jnp.exp(capped), 0.0), axis=-1, keepdims=True))
    probs = jnp.where(allowed, jnp.exp(capped - log_total), 0.0)
    probs_low = low(probs)
    mixed = jnp.einsum("bqk,bkd->bqd", probs_low, value, preferred_element_type=jnp.float32)
    mixed_low = low(mixed).reshape(-1, HEAD_DIM)
    attn_part = matmul_nt(mixed_low, out_full)
    with label("attn_gather"):
        attn_near = plane_core_sum(attn_part)
        attn_out = plane_sum(attn_near)
    with label("gate_join"):
        gate_full = plane_ffn_join(after(gate_far, attn_near), place)
    with label("up_far"):
        up_far = plane_ffn_far(after(up_near, attn_near))
    scale_post = rms_scale(attn_out)
    hidden = resid + attn_out * scale_post * post_attention_gain
    scale_ffn = rms_scale(hidden)
    ffn_rows = low(hidden * scale_ffn * pre_feedforward_gain)

    with label("ffn_spread"):
        ffn_near = line_near(ffn_rows)
    with label("down_near"):
        down_near = plane_ffn_near(after(down_line, ffn_rows, up_near))
    with label("ffn_spread"):
        ffn_input = line_far(ffn_near)
    with label("up_join"):
        up_full = plane_ffn_join(up_far, place)
    gate_lin = matmul(ffn_input, gate_full)
    up_lin = matmul(ffn_input, up_full)
    gelu_value, gelu_slope = gelu_parts(gate_lin)
    product = low(gelu_value * up_lin)
    with label("down_far"):
        down_far = plane_ffn_far(after(down_near, ffn_input))
        down_full = plane_ffn_join(down_far, place)
    with label("ffn_gather"):
        ffn_out = line_sum(core_sum(matmul_nt(product, down_full)))
    scale_out = rms_scale(ffn_out)
    block_out = low(hidden + ffn_out * scale_out * post_feedforward_gain)

    upstream = wide(output_cotangent[0])
    grad_post_ffn = jnp.sum(upstream * ffn_out * scale_out, axis=0)
    d_ffn_rows = low(norm_back(upstream, ffn_out, scale_out, post_feedforward_gain))
    with label("d_ffn_spread"):
        d_ffn_out = line_far(line_near(d_ffn_rows))
    d_product = matmul(d_ffn_out, down_full)
    d_gate = low(d_product * up_lin * gelu_slope)
    d_up = low(d_product * gelu_value)
    ffn_part = matmul_nt(d_gate, gate_full) + matmul_nt(d_up, up_full)
    with label("d_ffn_gather"):
        near_sum = core_sum(ffn_part)
        d_ffn_input = line_sum(near_sum)
    down_part = low(matmul_tn(after(d_ffn_out, ffn_part), product))
    with label("down_back_near"):
        down_near = back_near(down_part, place)
    ffn_again = after(ffn_input, down_part, near_sum)
    gate_part = low(matmul_tn(ffn_again, d_gate))
    with label("down_back_far"):
        down_far = back_far(after(down_near, gate_part), place)
    with label("gate_back_near"):
        gate_near = back_near(after(gate_part, down_near), place)
    up_part = low(matmul_tn(after(ffn_again, gate_part), d_up))
    d_ffn_input = after(d_ffn_input, up_part, down_near)

    grad_pre_ffn = jnp.sum(d_ffn_input * hidden * scale_ffn, axis=0)
    d_hidden = upstream + norm_back(d_ffn_input, hidden, scale_ffn, pre_feedforward_gain)
    grad_post_attn = jnp.sum(d_hidden * attn_out * scale_post, axis=0)
    d_attn_rows = low(norm_back(d_hidden, attn_out, scale_post, post_attention_gain))
    with label("d_attn_spread"):
        d_attn_near = plane_near(d_attn_rows)
    with label("down_back_z"):
        down_sum = back_sum(after(down_far, d_attn_rows))
        down_grad = back_line(down_sum, place)
    with label("d_attn_spread"):
        d_attn_out = plane_far(after(d_attn_near, down_sum))
    out_part = low(matmul_tn(d_attn_out, mixed_low))
    with label("out_back_z"):
        out_sum = back_attn_line(out_part, place)
    d_mixed = per_seq(matmul(d_attn_out, out_full))
    d_mixed_low = low(d_mixed)
    delta = jnp.sum(d_mixed * mixed, axis=-1, keepdims=True)
    d_probs = jnp.einsum("bqd,bkd->bqk", d_mixed_low, value, preferred_element_type=jnp.float32)
    d_scores = low(probs * (d_probs - delta) * (1.0 - bent * bent))
    d_query = jnp.einsum("bqk,bkd->bqd", d_scores, key, preferred_element_type=jnp.float32)
    d_key = jnp.einsum("bqk,bqd->bkd", d_scores, query, preferred_element_type=jnp.float32)
    d_value = jnp.einsum("bqk,bqd->bkd", probs_low, d_mixed_low, preferred_element_type=jnp.float32)
    d_query_low = low(rotate(d_query.reshape(-1, HEAD_DIM), cosine, -sine) * query_scale)
    keep = jnp.where(x == 0, d_key, d_value).reshape(-1, HEAD_DIM)
    give = low(jnp.where(x == 0, d_value, d_key)).reshape(-1, HEAD_DIM)
    with label("kv_back"):
        far_give = swap(give, "x")
    with label("gate_back_far"):
        gate_far = back_far(after(gate_near, give), place)
    with label("up_back_near"):
        up_near = back_near(after(up_part, gate_near, give), place)
    d_kv = keep + wide(turned(after(far_give, gate_near)))
    d_kv_low = low(jnp.where(x == 0, rotate(d_kv, cosine, -sine), d_kv))
    d_qkv = jnp.concatenate([d_query_low, d_kv_low], 1)
    attn_part = matmul_nt(d_qkv, qkv_full)
    qkv_part = low(matmul_tn(after(attn_input, attn_part), d_qkv))
    with label("qkv_back_z"):
        qkv_sum = back_attn_line(qkv_part, place)
    with label("d_attn_gather"):
        near_sum = plane_core_sum(attn_part)
        d_attn_input = plane_sum(near_sum)
    with label("gate_back_z"):
        gate_sum = back_sum(after(gate_far, near_sum))
        gate_grad = back_line(gate_sum, place)
    with label("up_back_far"):
        up_far = back_far(after(up_near, gate_sum), place)
    with label("out_back_plane"):
        out_parts = back_attn_plane(after(out_sum, near_sum), place)
    d_attn_input = after(d_attn_input, gate_sum)
    grad_pre_attn = jnp.sum(d_attn_input * resid * scale_attn, axis=0)
    input_grad = low(d_hidden + norm_back(d_attn_input, resid, scale_attn, pre_attention_gain))

    with label("qkv_back_plane"):
        qkv_parts = back_attn_plane(qkv_sum, place)
    with label("up_back_z"):
        up_grad = back_line(back_sum(up_far), place)

    def ordered(parts):
        grid = jnp.stack(parts).reshape((2, 2) + parts[0].shape)
        grid = jnp.where(x == 0, grid, grid[::-1])
        return jnp.where(y == 0, grid, grid[:, ::-1])

    def heads(grid):
        return jnp.concatenate([grid[0, 0], grid[1, 0], grid[0, 1], grid[1, 1]], 1)

    output_grad = heads(ordered(out_parts))
    qkv_grid = ordered(qkv_parts)
    query_grad = heads(qkv_grid[..., :HEAD_DIM])
    rest = qkv_grid[..., HEAD_DIM:]
    key_grad = jnp.concatenate([rest[0, 0], rest[0, 1]], 1)
    value_grad = jnp.concatenate([rest[1, 0], rest[1, 1]], 1)

    with label("gains"):
        gain_sums = sum_everywhere(
            jnp.stack([grad_pre_attn, grad_post_attn, grad_pre_ffn, grad_post_ffn])
        )
    return (
        block_out[None],
        input_grad[None],
        query_grad,
        key_grad,
        value_grad,
        output_grad,
        gate_grad,
        up_grad,
        down_grad,
        gain_sums[0],
        gain_sums[1],
        gain_sums[2],
        gain_sums[3],
    )


def solution(mesh):
    dp, ctx, tensor = (mesh.shape[name] for name in ("dp", "ctx", "tensor"))
    shape = (LINE, dp // (LINE * PAIR), PAIR, ctx, tensor)
    fine = Mesh(mesh.devices.reshape(shape), ("z", "m", "x", "y", "c"))
    seqs = ("z", "m", "x")
    tokens = P(seqs, ("y", "c"), None)
    weight = P(seqs + ("y",), "c")
    in_specs = (tokens, P(seqs, None), P(seqs, None)) + (weight,) * 7 + (P(),) * 4 + (tokens,)
    out_specs = (tokens, tokens) + (weight,) * 7 + (P(),) * 4
    return jax.shard_map(body, mesh=fine, in_specs=in_specs, out_specs=out_specs, check_vma=False)
```
